32 devices in a mesh: dp: 8 (over y, x, core), mp: 4 (over z).
Axes of the slice: x: 2, y: 2, z: 4, core: 2. Of those that a mesh axis runs over, the one named last changes fastest.
Arguments:
- replay_deter: bfloat16 [1024, 2048], P('dp', 'mp'), may hold values from -4 to 4
- permutation: int32 [1024], replicated, may hold values from 0 to 1023, as said below
- stoch_index: int32 [5, 32, 1024], P(None, 'mp', 'dp'), may hold values from 0 to 31
- action_index: int32 [4, 1024], P(None, 'dp'), may hold values from 0 to 17
- cat_weight: bfloat16 [4, 512, 2048], P('mp', 'dp'), may hold values from -0.125 to 0.125
- gru_weight: bfloat16 [4, 1536, 1536], P('mp', 'dp'), may hold values from -0.15625 to 0.15625
- stoch_weight: bfloat16 [32, 32, 1024], P('mp'), may hold values from -1 to 1
- action_embed: bfloat16 [18, 1024], replicated, may hold values from -6 to 6
- prior_weight: bfloat16 [1024, 1024], P(None, 'mp'), may hold values from -0.375 to 0.375
- input_gain: float32 [1024], replicated, may hold values from 0.1 to 1.9
- prior_gain: float32 [1024], replicated, may hold values from 0.1 to 1.9
Outputs:
- final_deter: float32 [1024, 2048], P('dp', 'mp')
- log_prob: float32 [4, 32, 1024], P(None, 'mp', 'dp')
- entropy: float32 [4, 32, 1024], P(None, 'mp', 'dp')
The draws below stay inside these ranges and needn't reach their ends.
Inputs may be any that keep to these rules, and one draw needn't show every extreme that they name: A permutation of the rows; for every block of 128 rollout rows and every block of 128 replay rows, the same number of the rollout rows take their replay row from that block.
All inputs are finite; a program needn't handle non-finite values.
Results may differ from the reference program's by a relative error of at most 0.0065.
Values may be sent and summed in bfloat16 or wider, within the bound.
No kernel may reach another device: no remote copies, remote signals or barrier semaphores. Data moves between devices by JAX's collectives and lax.ppermute only.
A program may use at most 64 MiB of HBM per device.

```python
import jax
import jax.numpy as jnp
from jax import lax

START_DEV = 128
BLK = 512
HIDDEN_SIZE = 1024
GROUPS = 32
CLASSES = 32
ACTIONS = 18
STEPS = 4
STARTS = 1024
BLOCKS = 4
DETER = 2048


def draw_permutation(key, part):
    block_count = STARTS // START_DEV
    share_count = START_DEV // block_count
    first_key, second_key = jax.random.split(key)
    source_rows = jax.vmap(lambda sub_key: jax.random.permutation(sub_key, START_DEV))(jax.random.split(first_key, block_count))
    source_rows = source_rows + (jnp.arange(block_count, dtype=jnp.int32) * START_DEV)[:, None]
    source_rows = source_rows.reshape(block_count, block_count, share_count)
    target_rows = jnp.transpose(source_rows, (1, 0, 2)).reshape(block_count, START_DEV)
    shuffled = jax.vmap(lambda sub_key, row_values: jax.random.permutation(sub_key, row_values))(jax.random.split(second_key, block_count), target_rows)
    return shuffled.reshape(STARTS).astype(jnp.int32)


def with_ends(entries, key, low, largest):
    longest = entries.shape.index(max(entries.shape))
    spots = []
    for shift in (0, 1):
        where = [jax.random.randint(jax.random.fold_in(key, axis), (), 0, length) for axis, length in enumerate(entries.shape)]
        where[longest] = (where[longest] + shift) % entries.shape[longest]
        spots.append(tuple(where))
    return entries.at[spots[0]].set(low).at[spots[1]].set(largest)


def block_levels(key, shape, cuts, low, top_value):
    gain, own = 1.0, jax.random.fold_in(key, 6)
    for dim, shards_of in cuts:
        heights = jnp.exp(jax.random.uniform(jax.random.fold_in(own, dim), (shards_of,), jnp.float32, low / len(cuts), top_value / len(cuts)))
        gain = gain * jnp.repeat(heights, shape[dim] // shards_of).reshape([-1 if axis == dim else 1 for axis in range(len(shape))])
    return gain


def gaussian(own_key, extent, deviation, limit, pieces=(), kind=jnp.bfloat16):
    result = jax.random.normal(own_key, extent, jnp.float32) * deviation
    if len(pieces) > 0:
        result = block_levels(own_key, extent, pieces, -0.22, 0.18) * result
    return jnp.clip(result, min=-limit, max=limit).astype(kind)


def setup_inputs(seed: int = 0) -> dict:
    splits = jax.random.split(jax.random.key(seed), 12)
    return {
        "replay_deter": gaussian(splits[0], (STARTS, DETER), 1.0, 4.0, ((0, 8), (1, 4))),
        "permutation": draw_permutation(jax.random.fold_in(splits[11], 71), 0),
        "stoch_index": with_ends(jax.random.randint(splits[2], (STEPS + 1, GROUPS, STARTS), 0, CLASSES), jax.random.fold_in(splits[2], 1), 0, CLASSES - 1).astype(jnp.int32),
        "action_index": with_ends(jax.random.randint(splits[3], (STEPS, STARTS), 0, ACTIONS), jax.random.fold_in(splits[3], 1), 0, ACTIONS - 1).astype(jnp.int32),
        "cat_weight": gaussian(splits[4], (BLOCKS, BLK, 2 * HIDDEN_SIZE), DETER ** -0.5, 0.125, ((0, 4), (1, 8))),
        "gru_weight": gaussian(splits[5], (BLOCKS, BLK + HIDDEN_SIZE, 3 * BLK), (BLK + HIDDEN_SIZE) ** -0.5, 0.15625, ((0, 4), (1, 8))),
        "stoch_weight": gaussian(splits[6], (GROUPS, CLASSES, HIDDEN_SIZE), GROUPS ** -0.5, 1.0, ((0, 4),)),
        "action_embed": gaussian(splits[7], (ACTIONS, HIDDEN_SIZE), 1 ** -0.5, 6.0),
        "prior_weight": gaussian(splits[8], (HIDDEN_SIZE, GROUPS * CLASSES), (HIDDEN_SIZE // 4) ** -0.5, 0.375, ((1, 4),)),
        "input_gain": jnp.clip(1.0 + 0.18 * jax.random.normal(splits[9], (HIDDEN_SIZE,), jnp.float32), 0.1, 1.9),
        "prior_gain": jnp.clip(1.0 + 0.18 * jax.random.normal(splits[10], (HIDDEN_SIZE,), jnp.float32), 0.1, 1.9),
    }


epsilon = 1e-06
mix_share = 0.01

def normed_silu(values, gain_vector):
    inverse_rms = lax.rsqrt(lax.optimization_barrier(jnp.mean(values * values, axis=-1, keepdims=True)) + epsilon)
    return jax.nn.silu(values * inverse_rms * gain_vector).astype(jnp.bfloat16)

def next_state(recurrent, gate_values):
    state_width = recurrent.shape[1]
    reset_gate = jax.nn.sigmoid(gate_values[:, :state_width])
    candidate = jnp.tanh(reset_gate * gate_values[:, state_width:2 * state_width])
    update = jax.nn.sigmoid(gate_values[:, 2 * state_width:] - 1.0)
    return update * candidate + (1.0 - update) * recurrent

def prior_terms(summed, gain_vector, table, chosen_hot, class_count):
    hidden = normed_silu(summed, gain_vector)
    logits = jnp.dot(hidden, table, preferred_element_type=jnp.float32)
    logits = logits.reshape(logits.shape[0], -1, class_count)
    weights = jnp.exp(logits)
    probabilities = (1.0 - mix_share) * weights / lax.optimization_barrier(jnp.sum(weights, axis=-1, keepdims=True)) + mix_share / class_count
    log_probs = jnp.log(probabilities)
    picked = lax.optimization_barrier(jnp.sum(jnp.where(chosen_hot, log_probs, 0.0), axis=-1))
    spread = -lax.optimization_barrier(jnp.sum(probabilities * log_probs, axis=-1))
    return (picked.T, spread.T)

def to_wire(values):
    return lax.optimization_barrier(values.astype(jnp.bfloat16)).astype(jnp.float32)

def reference(replay_deter, permutation, stoch_index, action_index, cat_weight, gru_weight, stoch_weight, action_embed, prior_weight, input_gain, prior_gain):
    group_share = GROUPS // BLOCKS
    span_width = group_share * CLASSES
    classes = jnp.arange(CLASSES, dtype=jnp.int32)
    stoch_table = stoch_weight.reshape(GROUPS * CLASSES, HIDDEN_SIZE)
    recurrent = jnp.take(replay_deter, permutation, axis=0).astype(jnp.float32)
    picked_all = []
    spread_all = []
    for step_number in range(STEPS + 1):
        state_bf = recurrent.astype(jnp.bfloat16)
        chosen_hot = jnp.transpose(stoch_index[step_number])[:, :, None] == classes
        stoch_flat = chosen_hot.reshape(STARTS, GROUPS * CLASSES).astype(jnp.bfloat16)
        input_sum = jnp.zeros((STARTS, HIDDEN_SIZE), jnp.float32)
        prior_sum = jnp.zeros((STARTS, HIDDEN_SIZE), jnp.float32)
        for block_index in range(BLOCKS):
            state_rows = state_bf[:, block_index * BLK:(block_index + 1) * BLK]
            if step_number < STEPS:
                block_part = jnp.dot(state_rows, cat_weight[block_index][:, :HIDDEN_SIZE], preferred_element_type=jnp.float32)
                block_part = block_part + jnp.dot(stoch_flat[:, block_index * span_width:(block_index + 1) * span_width], stoch_table[block_index * span_width:(block_index + 1) * span_width], preferred_element_type=jnp.float32)
                input_sum = input_sum + to_wire(block_part)
            if step_number > 0:
                prior_part = jnp.dot(state_rows, cat_weight[block_index][:, HIDDEN_SIZE:], preferred_element_type=jnp.float32)
                prior_sum = prior_sum + to_wire(prior_part)
        if step_number > 0:
            picked, spread = prior_terms(prior_sum, prior_gain, prior_weight, chosen_hot, CLASSES)
            picked_all.append(picked)
            spread_all.append(spread)
        if step_number < STEPS:
            action_rows = jnp.take(action_embed, action_index[step_number], axis=0).astype(jnp.float32)
            gru_input = normed_silu(input_sum + action_rows, input_gain)
            new_blocks = []
            for block_index in range(BLOCKS):
                state_rows = state_bf[:, block_index * BLK:(block_index + 1) * BLK]
                inputs = jnp.concatenate([state_rows, gru_input], axis=1)
                gate_values = jnp.dot(inputs, gru_weight[block_index], preferred_element_type=jnp.float32)
                new_blocks.append(next_state(recurrent[:, block_index * BLK:(block_index + 1) * BLK], gate_values))
            recurrent = jnp.concatenate(new_blocks, axis=1)
    return (recurrent, jnp.stack(picked_all), jnp.stack(spread_all))
```

```python
import functools

import jax
import jax.numpy as jnp
from jax import lax
from jax.experimental import pallas as pl
from jax.experimental.pallas import tpu as pltpu
from jax.sharding import PartitionSpec as P

epsilon = 1e-06
mix_share = 0.01
row_tile = 16


vmem = pl.BlockSpec(memory_space=pltpu.VMEM)
smem = pl.BlockSpec(memory_space=pltpu.SMEM)
anywhere = pl.BlockSpec(memory_space=pl.ANY)
params = pltpu.CompilerParams(vmem_limit_bytes=40 << 20)


def call(body, name, in_specs, out_specs, out_shape, scratch=()):
    return pl.pallas_call(
        body,
        name=name,
        in_specs=in_specs,
        out_specs=out_specs,
        out_shape=out_shape,
        scratch_shapes=list(scratch),
        compiler_params=params,
    )


def f32_dot(a, b):
    return jnp.dot(a, b, preferred_element_type=jnp.float32)


def across(a, b):
    return lax.dot_general(a, b, (((1,), (1,)), ((), ())), preferred_element_type=jnp.float32)


def swap(value, bit, axis="dp"):
    count = lax.axis_size(axis)
    return lax.ppermute(value, axis, [(i, i ^ bit) for i in range(count)])


def exchange(pieces, axis="mp"):
    count = lax.axis_size(axis)
    moved = [pieces[0]]
    for shift in range(1, count):
        moved.append(
            lax.ppermute(pieces[shift], axis, [(i, (i + shift) % count) for i in range(count)])
        )
    return moved


def spread(shard):
    count = lax.axis_size("dp")
    half = shard.shape[0] // 2
    if count & (count - 1) or half % row_tile or count < 4:
        return [(None, 0, lax.all_gather(shard, "dp", axis=0, tiled=True))]
    bits = [1 << b for b in range(count.bit_length() - 1)]
    core, links = bits[0], bits[1:]
    got = {0: [(0, shard)]}
    for bit in links:
        got[bit] = [(0, swap(shard, bit))]

    def part(entries, second):
        if len(entries) == 2:
            return entries[second][1]
        return entries[0][1][half:] if second else entries[0][1][:half]

    for key in sorted(range(0, count, 2), key=lambda k: bin(k).count("1")):
        if key in got:
            continue
        low, high = key & -key, 1 << (key.bit_length() - 1)
        got[key] = [
            (0, swap(part(got[key ^ high], 0), high)),
            (half, swap(part(got[key ^ low], 1), low)),
        ]
    for key in list(got):
        got[key | core] = [(offset, swap(rows, core)) for offset, rows in got[key]]
    return [(key, offset, rows) for key in sorted(got) for offset, rows in got[key]]


def landing(entry, refs, ids, shard_rows, target, sems):
    copies = []
    for index, ((key, offset, shape), ref) in enumerate(zip(entry, refs)):
        if key is None:
            place = target
        else:
            start = pl.multiple_of((ids[0] ^ key) * shard_rows + offset, row_tile)
            place = target.at[pl.ds(start, shape[0]), :]
        copies.append(pltpu.make_async_copy(ref, place, sems.at[index]))
    return copies


def send_rows(perm, ids, replay):
    block_count, row_count = perm.shape
    share = row_count // block_count

    def body(ids_ref, perm_ref, replay_ref, out_ref):
        base = ids_ref[0] * row_count
        local = perm_ref[...] - base
        mine = jnp.logical_and(local >= 0, local < row_count)
        before = lax.broadcasted_iota(jnp.int32, (row_count, row_count), 0) < lax.broadcasted_iota(
            jnp.int32, (row_count, row_count), 1
        )
        rank = f32_dot(
            jnp.where(mine, 1.0, 0.0).astype(jnp.bfloat16),
            jnp.where(before, 1.0, 0.0).astype(jnp.bfloat16),
        ).astype(jnp.int32)
        rank = jnp.where(mine, rank, -1)
        slots = lax.broadcasted_iota(jnp.int32, (share, row_count), 0)
        sources = lax.broadcasted_iota(jnp.int32, (row_count, row_count), 0)
        for block in range(block_count):
            takes = jnp.where(rank[block : block + 1] == slots, 1.0, 0.0).astype(jnp.bfloat16)
            holds = jnp.where(local[block : block + 1] == sources, 1.0, 0.0).astype(jnp.bfloat16)
            chosen = across(takes, holds).astype(jnp.bfloat16)
            out_ref[block] = f32_dot(chosen, replay_ref[...]).astype(jnp.bfloat16)

    shape = jax.ShapeDtypeStruct((block_count, share, replay.shape[1]), jnp.bfloat16)
    return call(body, "send_rows", [smem, vmem, vmem], vmem, shape)(ids, perm, replay)


def place_rows(own_perm, incoming):
    row_count = own_perm.shape[1]
    block_count, share, width = incoming.shape

    def body(perm_ref, in_ref, out_ref):
        source = perm_ref[...] // row_count
        blocks = lax.broadcasted_iota(jnp.int32, (block_count, row_count), 0)
        match = jnp.where(source == blocks, 1.0, 0.0)
        before = lax.broadcasted_iota(jnp.int32, (row_count, row_count), 0) < lax.broadcasted_iota(
            jnp.int32, (row_count, row_count), 1
        )
        rank = f32_dot(
            match.astype(jnp.bfloat16), jnp.where(before, 1.0, 0.0).astype(jnp.bfloat16)
        )
        rank = jnp.sum(rank * match, axis=0, keepdims=True).astype(jnp.int32)
        slot = source * share + rank
        slots = lax.broadcasted_iota(jnp.int32, (row_count, row_count), 0)
        chosen = jnp.where(slot == slots, 1.0, 0.0).T.astype(jnp.bfloat16)
        out_ref[...] = f32_dot(chosen, in_ref[...].reshape(row_count, width)).astype(jnp.bfloat16)

    shape = jax.ShapeDtypeStruct((row_count, width), jnp.bfloat16)
    return call(body, "place_rows", [vmem, vmem], vmem, shape)(own_perm, incoming)


def replayed(replay, permutation, ids):
    row_count, width = replay.shape
    block_count = lax.axis_size("dp")
    share = row_count // block_count
    rank = lax.axis_index("dp")
    own = lax.dynamic_slice_in_dim(permutation, rank * row_count, row_count)
    if share % row_tile == 0:
        outgoing = send_rows(permutation.reshape(block_count, row_count), ids, replay)
        incoming = lax.all_to_all(outgoing, "dp", split_axis=0, concat_axis=0, tiled=True)
        return place_rows(own[None], incoming)
    inverse = jnp.argsort(permutation)
    targets = lax.dynamic_slice_in_dim(inverse, rank * row_count, row_count)
    outgoing = jnp.take(replay, jnp.argsort(targets), axis=0)
    incoming = lax.all_to_all(
        outgoing.reshape(block_count, share, width), "dp", split_axis=0, concat_axis=0, tiled=True
    )
    keys = own // row_count * row_count + jnp.arange(row_count, dtype=jnp.int32)
    placed = jnp.argsort(jnp.argsort(keys))
    return jnp.take(incoming.reshape(row_count, width), placed, axis=0)


def part_shapes(part_count, share, width):
    return [jax.ShapeDtypeStruct((share, width), jnp.bfloat16)] * part_count


def write_parts(part, held, ids, outs):
    held[...] = part
    count = len(outs)
    share = outs[0].shape[0]
    for shift, out in enumerate(outs):
        start = pl.multiple_of(lax.rem(ids[1] + shift, count) * share, share)
        out[...] = held[pl.ds(start, share), :].astype(jnp.bfloat16)


def read_parts(refs, held, ids):
    count = len(refs)
    share = refs[0].shape[0]
    for shift, ref in enumerate(refs):
        start = pl.multiple_of(lax.rem(ids[1] + count - shift, count) * share, share)
        held[pl.ds(start, share), :] = ref[...].astype(held.dtype)
    return held[...].astype(jnp.bfloat16)


def row_dtype(share):
    return jnp.bfloat16 if share % row_tile == 0 else jnp.float32


def first_parts(ids, state, hot, table, cat, shard_rows, part_count):
    row_count, width = state.shape
    hidden = table.shape[1]
    share = row_count // part_count
    entry = [(key, offset, rows.shape) for key, offset, rows in cat]
    n_cat = len(cat)

    def body(*refs):
        ids_ref, state_ref, hot_ref, table_ref = refs[:4]
        cat_refs = refs[4 : 4 + n_cat]
        whole_ref = refs[4 + n_cat]
        outs = refs[5 + n_cat : 5 + n_cat + part_count]
        held, whole, sems, out_sem = refs[5 + n_cat + part_count :]
        copies = landing(entry, cat_refs, ids_ref, shard_rows, whole, sems)
        for copy in copies:
            copy.start()
        part = f32_dot(hot_ref[...], table_ref[...])
        for copy in copies:
            copy.wait()
        back = pltpu.make_async_copy(whole, whole_ref, out_sem.at[0])
        back.start()
        part = f32_dot(state_ref[...], whole[:, :hidden]) + part
        write_parts(part, held, ids_ref, outs)
        back.wait()

    result = call(
        body,
        "first_parts",
        [smem, vmem, vmem, vmem] + [anywhere] * n_cat,
        [anywhere] + [vmem] * part_count,
        [jax.ShapeDtypeStruct((width, 2 * hidden), jnp.bfloat16)]
        + part_shapes(part_count, share, hidden),
        [
            pltpu.VMEM((row_count, hidden), jnp.float32),
            pltpu.VMEM((width, 2 * hidden), jnp.bfloat16),
            pltpu.SemaphoreType.DMA((n_cat,)),
            pltpu.SemaphoreType.DMA((1,)),
        ],
    )(ids, state, hot, table, *[rows for _, _, rows in cat])
    return result[0], list(result[1:])


def updated(gates, recurrent):
    width = recurrent.shape[1]
    reset = jax.nn.sigmoid(gates[:, :width])
    cand = jnp.tanh(reset * gates[:, width : 2 * width])
    update = jax.nn.sigmoid(gates[:, 2 * width :] - 1.0)
    return update * cand + (1.0 - update) * recurrent


def first_step(ids, xs, state, gru, hot, table, cat, shard_rows):
    row_count, width = state.shape
    hidden = table.shape[1]
    part_count = len(xs)
    share = row_count // part_count
    entry = [(key, offset, rows.shape) for key, offset, rows in gru]
    n_gru = len(gru)
    n_in = 5 + part_count

    def body(*refs):
        ids_ref, state_ref, hot_ref, table_ref = refs[:4]
        x_refs = refs[4 : 4 + part_count]
        cat_ref = refs[4 + part_count]
        gru_refs = refs[n_in : n_in + n_gru]
        whole_ref, deter_ref, bf_ref = refs[n_in + n_gru : n_in + n_gru + 3]
        outs = refs[n_in + n_gru + 3 : n_in + n_gru + 3 + part_count]
        x_held, held, whole, cat_in, sems, out_sem = refs[n_in + n_gru + 3 + part_count :]
        copies = landing(entry, gru_refs, ids_ref, shard_rows, whole, sems)
        for copy in copies:
            copy.start()
        cat_copy = pltpu.make_async_copy(cat_ref.at[:, pl.ds(0, hidden)], cat_in, out_sem.at[1])
        cat_copy.start()
        x = read_parts(x_refs, x_held, ids_ref)
        part = f32_dot(hot_ref[...], table_ref[...])
        for copy in copies:
            copy.wait()
        back = pltpu.make_async_copy(whole, whole_ref, out_sem.at[0])
        back.start()
        state_bf = state_ref[...]
        gates = f32_dot(state_bf, whole[:width, :]) + f32_dot(x, whole[width:, :])
        deter = updated(gates, state_bf.astype(jnp.float32))
        deter_ref[...] = deter
        deter_bf = deter.astype(jnp.bfloat16)
        bf_ref[...] = deter_bf
        cat_copy.wait()
        part = f32_dot(deter_bf, cat_in[...]) + part
        write_parts(part, held, ids_ref, outs)
        back.wait()

    total = width + hidden
    result = call(
        body,
        "first_step",
        [smem] + [vmem] * (3 + part_count) + [anywhere] * (1 + n_gru),
        [anywhere] + [vmem] * (2 + part_count),
        [
            jax.ShapeDtypeStruct((total, 3 * width), jnp.bfloat16),
            jax.ShapeDtypeStruct((row_count, width), jnp.float32),
            jax.ShapeDtypeStruct((row_count, width), jnp.bfloat16),
        ]
        + part_shapes(part_count, share, hidden),
        [
            pltpu.VMEM((row_count, hidden), row_dtype(share)),
            pltpu.VMEM((row_count, hidden), jnp.float32),
            pltpu.VMEM((total, 3 * width), jnp.bfloat16),
            pltpu.VMEM((width, hidden), jnp.bfloat16),
            pltpu.SemaphoreType.DMA((n_gru,)),
            pltpu.SemaphoreType.DMA((2,)),
        ],
    )(ids, state, hot, table, *xs, cat, *[rows for _, _, rows in gru])
    return result[0], result[1], result[2], list(result[3:])


def next_step(ids, xs, deter, state_gates, gru, cat, hot=None, table=None):
    row_count, width = deter.shape
    hidden = cat.shape[1] // 2
    part_count = len(xs)
    share = row_count // part_count
    inner = hot is not None
    extra = [hot, table] if inner else []
    n_in = 3 + part_count + len(extra)

    def body(*refs):
        ids_ref, deter_ref, gates_ref = refs[:3]
        x_refs = refs[3 : 3 + part_count]
        extra_refs = refs[3 + part_count : n_in]
        gru_ref, cat_ref = refs[n_in : n_in + 2]
        new_ref = refs[n_in + 2]
        count = 2 if inner else 1
        outs = refs[n_in + 2 + count : n_in + 2 + count + part_count]
        x_held, held, rows_x, cat_half, sems = refs[n_in + 2 + count + part_count :]
        copies = []
        for gate in range(3):
            span = pl.ds(gate * width, width)
            copies.append(
                pltpu.make_async_copy(
                    gru_ref.at[pl.ds(width, hidden), span], rows_x.at[:, span], sems.at[gate]
                )
            )
        copies.append(
            pltpu.make_async_copy(
                cat_ref.at[:, pl.ds(0 if inner else hidden, hidden)], cat_half, sems.at[3]
            )
        )
        for copy in copies:
            copy.start()
        x = read_parts(x_refs, x_held, ids_ref)

        def gate_of(gate):
            copies[gate].wait()
            span = slice(gate * width, (gate + 1) * width)
            return f32_dot(x, rows_x[:, span]) + gates_ref[:, span]

        reset = jax.nn.sigmoid(gate_of(0))
        cand = jnp.tanh(reset * gate_of(1))
        update = jax.nn.sigmoid(gate_of(2) - 1.0)
        new = update * cand + (1.0 - update) * deter_ref[...]
        new_ref[...] = new
        new_bf = new.astype(jnp.bfloat16)
        copies[3].wait()
        part = f32_dot(new_bf, cat_half[...])
        if inner:
            refs[n_in + 3][...] = new_bf
            part = part + f32_dot(extra_refs[0][...], extra_refs[1][...])
        write_parts(part, held, ids_ref, outs)

    shapes = [jax.ShapeDtypeStruct((row_count, width), jnp.float32)]
    if inner:
        shapes.append(jax.ShapeDtypeStruct((row_count, width), jnp.bfloat16))
    shapes += part_shapes(part_count, share, hidden)
    result = call(
        body,
        "next_step" if inner else "last_step",
        [smem] + [vmem] * (n_in - 1) + [anywhere] * 2,
        [vmem] * len(shapes),
        shapes,
        [
            pltpu.VMEM((row_count, hidden), row_dtype(share)),
            pltpu.VMEM((row_count, hidden), jnp.float32),
            pltpu.VMEM((hidden, 3 * width), jnp.bfloat16),
            pltpu.VMEM((width, hidden), jnp.bfloat16),
            pltpu.SemaphoreType.DMA((4,)),
        ],
    )(ids, deter, state_gates, *xs, *extra, gru, cat)
    if inner:
        return result[0], result[1], list(result[2:])
    return result[0], None, list(result[1:])


def beside(ids, state, gru, cat, part_count):
    row_count, width = state.shape
    hidden = cat.shape[1] // 2
    share = row_count // part_count

    def body(*refs):
        ids_ref, state_ref, gru_ref, cat_ref, gates_ref = refs[:5]
        outs = refs[5 : 5 + part_count]
        held, rows_s, cat_half, sems = refs[5 + part_count :]
        copies = [
            pltpu.make_async_copy(cat_ref.at[:, pl.ds(hidden, hidden)], cat_half, sems.at[0]),
            pltpu.make_async_copy(gru_ref.at[pl.ds(0, width), :], rows_s, sems.at[1]),
        ]
        for copy in copies:
            copy.start()
        copies[0].wait()
        write_parts(f32_dot(state_ref[...], cat_half[...]), held, ids_ref, outs)
        copies[1].wait()
        gates_ref[...] = f32_dot(state_ref[...], rows_s[...])

    result = call(
        body,
        "beside",
        [smem, vmem, anywhere, anywhere],
        [vmem] * (1 + part_count),
        [jax.ShapeDtypeStruct((row_count, 3 * width), jnp.float32)]
        + part_shapes(part_count, share, hidden),
        [
            pltpu.VMEM((row_count, hidden), jnp.float32),
            pltpu.VMEM((width, 3 * width), jnp.bfloat16),
            pltpu.VMEM((width, hidden), jnp.bfloat16),
            pltpu.SemaphoreType.DMA((2,)),
        ],
    )(ids, state, gru, cat)
    return result[0], list(result[1:])


def normed(parts, gain, action_rows=None):
    extra = [] if action_rows is None else [action_rows]
    count = len(parts)

    def body(*refs):
        total = refs[0][...].astype(jnp.float32)
        for ref in refs[1:count]:
            total = total + ref[...].astype(jnp.float32)
        if extra:
            total = total + refs[count + 1][...].astype(jnp.float32)
        inverse = lax.rsqrt(jnp.mean(total * total, axis=-1, keepdims=True) + epsilon)
        scaled = total * inverse * refs[count][...]
        refs[-1][...] = (scaled * jax.nn.sigmoid(scaled)).astype(jnp.bfloat16)

    return call(
        body,
        "normed",
        [vmem] * (count + 1 + len(extra)),
        vmem,
        jax.ShapeDtypeStruct(parts[0].shape, jnp.bfloat16),
    )(*parts, gain, *extra)


def prior_terms(ids, hidden_parts, table, chosen, class_count):
    group_count, row_count = chosen.shape
    part_count = len(hidden_parts)
    share, hidden = hidden_parts[0].shape

    def body(*refs):
        ids_ref, table_ref, chosen_ref = refs[:3]
        h_refs = refs[3 : 3 + part_count]
        picked_ref, spread_ref, h_held = refs[3 + part_count :]
        rows = read_parts(h_refs, h_held, ids_ref)
        logits = across(table_ref[...], rows).reshape(group_count, class_count, row_count)
        weights = jnp.exp(logits)
        total = jnp.sum(weights, axis=1, keepdims=True)
        probs = (1.0 - mix_share) * weights / total + mix_share / class_count
        logs = jnp.log(probs)
        spread_ref[...] = -jnp.sum(probs * logs, axis=1)
        classes = lax.broadcasted_iota(jnp.int32, logits.shape, 1)
        hit = classes == chosen_ref[...][:, None, :]
        picked_ref[...] = jnp.sum(jnp.where(hit, logs, 0.0), axis=1)

    shape = jax.ShapeDtypeStruct((group_count, row_count), jnp.float32)
    return call(
        body,
        "prior_terms",
        [smem] + [vmem] * (2 + part_count),
        [vmem, vmem],
        [shape, shape],
        [pltpu.VMEM((row_count, hidden), row_dtype(share))],
    )(ids, table, chosen, *hidden_parts)


def shards(
    replay_deter,
    permutation,
    stoch_index,
    action_index,
    cat_weight,
    gru_weight,
    stoch_weight,
    action_embed,
    prior_weight,
    input_gain,
    prior_gain,
):
    row_count, width = replay_deter.shape
    action_count, hidden = action_embed.shape
    group_count, class_count, _ = stoch_weight.shape
    step_count = action_index.shape[0]
    part_count = lax.axis_size("mp")
    share = row_count // part_count
    ids = jnp.stack([lax.axis_index("dp"), lax.axis_index("mp")]).astype(jnp.int32)

    cat = spread(cat_weight[0])
    state = replayed(replay_deter, permutation, ids)
    gru = spread(gru_weight[0])

    classes = jnp.arange(class_count, dtype=jnp.int32)
    hot = (jnp.transpose(stoch_index[:step_count], (0, 2, 1))[..., None] == classes).reshape(
        step_count, row_count, group_count * class_count
    )
    hot = hot.astype(jnp.bfloat16)
    table = stoch_weight.reshape(group_count * class_count, hidden)
    own_actions = lax.dynamic_slice_in_dim(
        action_index, lax.axis_index("mp") * share, share, axis=1
    )
    action_hot = own_actions[..., None] == jnp.arange(action_count, dtype=jnp.int32)
    action_rows = f32_dot(action_hot.astype(jnp.bfloat16), action_embed)
    prior_table = prior_weight.T
    input_gain = input_gain[None]
    prior_gain = prior_gain[None]

    picked_all = []
    spread_all = []

    def prior_step(parts, number):
        own = normed(exchange(parts), prior_gain)
        hidden_parts = exchange([own] * part_count)
        picked, spread_of = prior_terms(
            ids, hidden_parts, prior_table, stoch_index[number], class_count
        )
        picked_all.append(picked)
        spread_all.append(spread_of)

    cat, parts = first_parts(ids, state, hot[0], table, cat, cat_weight.shape[1], part_count)
    deter = None
    for number in range(step_count):
        moved = exchange(parts)
        if number > 0:
            state_gates, prior_parts = beside(ids, state, gru, cat, part_count)
        x_own = normed(moved, input_gain, action_rows[number])
        xs = exchange([x_own] * part_count)
        if number == 0:
            gru, deter, state, parts = first_step(
                ids, xs, state, gru, hot[1], table, cat, gru_weight.shape[1]
            )
        else:
            prior_step(prior_parts, number)
            more = (hot[number + 1], table) if number + 1 < step_count else ()
            deter, state, parts = next_step(ids, xs, deter, state_gates, gru, cat, *more)
    prior_step(parts, step_count)
    return (deter, jnp.stack(picked_all), jnp.stack(spread_all))


def solution(mesh):
    in_specs = (
        P("dp", "mp"),
        P(),
        P(None, "mp", "dp"),
        P(None, "dp"),
        P("mp", "dp", None),
        P("mp", "dp", None),
        P("mp", None, None),
        P(),
        P(None, "mp"),
        P(),
        P(),
    )
    out_specs = (P("dp", "mp"), P(None, "mp", "dp"), P(None, "mp", "dp"))
    return jax.shard_map(shards, mesh=mesh, in_specs=in_specs, out_specs=out_specs, check_vma=False)
```
